32 devices in a mesh: groups: 2 (over y), expert: 4 (over z), tensor: 4 (over x, core).
Axes of the slice: x: 2, y: 2, z: 4, core: 2. Of those that a mesh axis runs over, the one named last changes fastest.
Arguments:
- tokens: bfloat16 [256, 4096], P(('groups', 'expert'), 'tensor'), parts along dimension 0, may hold values from -6 to 6
- expert_ids: int32 [256, 8], P(('groups', 'expert')), parts along dimension 0, may hold values from 0 to 63, all different within a row; in each aligned block of 32 rows (0 to 31, 32 to 63, ...) at most 8 rows name the same one
- gate_fixed: int32 [256, 8], P(('groups', 'expert')), parts along dimension 0, may hold values from 1 to 65535
- w_gate: bfloat16 [64, 4096, 768], P('expert', None, 'tensor'), may hold values from -0.09375 to 0.09375
- w_up: bfloat16 [64, 4096, 768], P('expert', None, 'tensor'), may hold values from -0.09375 to 0.09375
- w_down: bfloat16 [64, 768, 4096], P('expert', 'tensor'), may hold values from -0.21875 to 0.21875
Outputs:
- mixed: bfloat16 [256, 4096], P(('groups', 'expert'), 'tensor'), parts along dimension 0
The draws below stay inside these ranges and needn't reach their ends.
There are 2 independent parts, one for each index of `groups`. The reference program is written for one: setup_inputs(seed, part) draws one part's arguments, and reference() takes and returns one part's arrays. A program takes and returns all parts, laid end to end along the dimension named above; an argument that names none is the same for every part. Nothing has to cross between parts.
Inputs may be any that keep to these rules, and one draw needn't show every extreme that they name: `expert_ids`: each row names 8 different experts. Within the 32 rows of one index of the expert axis no expert is named more than 8 times, and in every draw some expert is named exactly 8 times in some such block.
All inputs are finite; a program needn't handle non-finite values.
Results may differ from the reference program's by a relative error of at most 0.014.
Values may be sent and summed in bfloat16 or wider, within the bound.
A program may use at most 128 MiB of HBM per device.

```python
import math
import jax
import jax.numpy as jnp
import numpy as np
from jax import lax

D = 4096
FF = 768
EXPERTS = 64
TOP = 8
TOK_DEV = 32
CAP = 8
TOKENS = 128
N_TENSOR = 4


def plant(result, rng, smallest, top_value):
    longest = result.shape.index(max(result.shape))
    spots = []
    for shift in (0, 1):
        where = [jax.random.randint(jax.random.fold_in(rng, axis), (), 0, length) for axis, length in enumerate(result.shape)]
        where[longest] = (where[longest] + shift) % result.shape[longest]
        spots.append(tuple(where))
    return result.at[spots[0]].set(smallest).at[spots[1]].set(top_value)


def block_scale(rng, extent, shards, least, top_value):
    factor_of, own = 1.0, jax.random.fold_in(rng, 6)
    for axis_at, parts in shards:
        steps = jnp.exp(jax.random.uniform(jax.random.fold_in(own, axis_at), (parts,), jnp.float32, least / len(shards), top_value / len(shards)))
        factor_of = factor_of * jnp.repeat(steps, extent[axis_at] // parts).reshape([-1 if axis == axis_at else 1 for axis in range(len(extent))])
    return factor_of


def deal_out(rng, own, number, rows, number_of, top, most, lean):
    order = jax.random.permutation(rng, number_of)
    crowded, usual = portions_of(number_of, rows * top, most, lean, True), portions_of(number_of, rows * top, most, lean, False)
    places = jnp.arange(number_of)

    def named(sizes, rotation):
        used = int((sizes > 0).sum())
        fixed = max(1, used // 4)
        shifted = fixed + (places - fixed + rotation * (used - fixed)) % max(1, number_of - fixed)
        return jnp.zeros((number_of,), jnp.int32).at[order[jnp.where(places < fixed, places, shifted)]].set(jnp.asarray(sizes, jnp.int32))

    sizes = jnp.where(number % 4 == 0, named(crowded, number // 4), named(usual, number - number // 4 - 1))
    mixed = jax.random.permutation(jax.random.fold_in(own, 3), number_of)
    source_of, sink = mixed[0:number_of // 2 * 2:2], mixed[1:number_of // 2 * 2:2]
    slack = jnp.minimum(sizes[source_of] - 1, most - sizes[sink]) // 2
    slack = jnp.where((source_of == order[0]) | (sink == order[0]) | (sizes[sink] == 0), 0, jnp.maximum(slack, 0))
    shifted = jax.random.randint(jax.random.fold_in(own, 4), (number_of // 2,), 0, 1 << 20) % (slack + 1)
    sizes = sizes.at[source_of].add(-shifted).at[sink].add(shifted)
    items = jnp.searchsorted(jnp.cumsum(sizes), jnp.arange(rows * top), side="right").astype(jnp.int32)
    table = items.reshape(top, rows).T
    table = table[jax.random.permutation(jax.random.fold_in(own, 1), rows)]
    rotation = jax.random.randint(jax.random.fold_in(own, 2), (rows, 1), 0, top)
    return jnp.take_along_axis(table, (jnp.arange(top)[None, :] + rotation) % top, axis=1)


def portions_of(amount, total, reach, skew, full):
    loads = [(1 << 20) // math.isqrt(rank ** skew) + 1 for rank in range(1, amount + 1)]
    largest = reach if full else min(reach, max(-(-total // amount), total * loads[0] // sum(loads)))
    least = 1 if total - largest >= amount - 1 else 0
    counts, rest = [largest] + [least] * (amount - 1), total - largest - least * (amount - 1)
    while rest > 0:
        free = [i for i in range(1, amount) if counts[i] < largest] or [i for i in range(1, amount) if counts[i] < reach]
        pool, left = sum([loads[i] for i in free]), rest
        for i in free:
            extra = min(reach - counts[i], max(1, left * loads[i] // pool), rest)
            counts[i] = counts[i] + extra
            rest = rest - extra
    return np.array(counts)


def gaussian(stream_key, extent, width, bound, pieces=(), kind=jnp.bfloat16):
    level = block_scale(stream_key, extent, pieces, -0.22, 0.18) if pieces else 1.0
    entries = jax.random.normal(stream_key, extent, jnp.float32) * width * level
    return jnp.minimum(jnp.maximum(entries, -bound), bound).astype(kind)


def setup_inputs(seed: int = 0, part: int = 0) -> dict:
    key_list = jax.random.split(jax.random.key(seed), 7)
    part_splits = jax.random.split(jax.random.fold_in(key_list[6], part), 7)
    tokens = gaussian(part_splits[0], (TOKENS, D), 1.0, 6.0, ((0, 4), (1, 4)))
    expert_ids_keys = jax.random.split(jax.random.fold_in(part_splits[1], 1), TOKENS // TOK_DEV)
    expert_ids_turns = jax.random.permutation(jax.random.fold_in(part_splits[1], 3), TOKENS // TOK_DEV)
    expert_ids = jax.vmap(lambda own, number: deal_out(jax.random.fold_in(part_splits[1], 2), own, number, TOK_DEV, EXPERTS, TOP, CAP, 2))(expert_ids_keys, expert_ids_turns).reshape((TOKENS, TOP))
    gate_fixed = plant(jax.random.randint(part_splits[2], (TOKENS, TOP), 1, 65536), jax.random.fold_in(part_splits[2], 1), 1, 65535).astype(jnp.int32)
    w_gate = gaussian(key_list[3], (EXPERTS, D, FF), D ** -0.5, 0.09375, ((0, 4), (2, 4)))
    w_up = gaussian(key_list[4], (EXPERTS, D, FF), D ** -0.5, 0.09375, ((0, 4), (2, 4)))
    w_down = gaussian(key_list[5], (EXPERTS, FF, D), FF ** -0.5, 0.21875, ((0, 4), (1, 4)))
    return dict(tokens=tokens, expert_ids=expert_ids, gate_fixed=gate_fixed, w_gate=w_gate, w_up=w_up, w_down=w_down)


def reference(tokens, expert_ids, gate_fixed, w_gate, w_up, w_down):
    weights = gate_fixed.astype(jnp.float32)
    gate_share = weights / jnp.sum(weights, axis=1, keepdims=True)
    group_width = FF // N_TENSOR

    def one_expert(running, expert_index):
        chosen = jnp.sum(jnp.where(expert_ids == expert_index, gate_share, jnp.zeros_like(gate_share)), axis=1)
        gate_proj = jnp.dot(tokens, w_gate[expert_index], preferred_element_type=jnp.float32)
        up_proj = jnp.dot(tokens, w_up[expert_index], preferred_element_type=jnp.float32)
        hidden = (jax.nn.silu(gate_proj) * up_proj).astype(jnp.bfloat16)
        down = w_down[expert_index]
        summed = jnp.zeros((tokens.shape[0], D), jnp.float32)
        for piece_index in range(N_TENSOR):
            lower = piece_index * group_width
            group_term = jnp.dot(hidden[:, lower:lower + group_width], down[lower:lower + group_width], preferred_element_type=jnp.float32)
            summed = summed + lax.optimization_barrier(group_term.astype(jnp.bfloat16)).astype(jnp.float32)
        expert_out = lax.optimization_barrier(summed.astype(jnp.bfloat16)).astype(jnp.float32)
        return running + chosen[:, None] * expert_out, None

    start = jnp.zeros((tokens.shape[0], D), jnp.float32)
    running, unused = lax.scan(one_expert, start, jnp.arange(EXPERTS, dtype=jnp.int32))
    return running.astype(jnp.bfloat16)
```

```python
import functools

import jax
import jax.numpy as jnp
from jax import lax
from jax.experimental import pallas as pl
from jax.experimental.pallas import tpu as pltpu
from jax.sharding import PartitionSpec as P

CAP = 8


def expert_block(slot_rows, w_gate, w_up, w_down):
    gate_proj = jnp.einsum("gekd,edf->gekf", slot_rows, w_gate, preferred_element_type=jnp.float32)
    up_proj = jnp.einsum("gekd,edf->gekf", slot_rows, w_up, preferred_element_type=jnp.float32)
    hidden = (jax.nn.silu(gate_proj) * up_proj).astype(jnp.bfloat16)
    partial_value = jnp.einsum("gekf,efd->gekd", hidden, w_down, preferred_element_type=jnp.float32)
    summed = lax.psum_scatter(
        partial_value.astype(jnp.bfloat16), "tensor", scatter_dimension=3, tiled=True
    )
    return lax.all_to_all(summed, "expert", split_axis=0, concat_axis=0, tiled=True)


def slotted(tokens, expert_ids, gate_fixed, w_gate, w_up, w_down):
    tok_rows, per_token = expert_ids.shape
    local_experts = w_gate.shape[0]
    devices_e = lax.axis_size("expert")
    experts = local_experts * devices_e
    capacity = CAP
    flat_ids = expert_ids.reshape(-1)
    pick_count = tok_rows * per_token
    onehot = (flat_ids[:, None] == jnp.arange(experts, dtype=jnp.int32)[None, :]).astype(jnp.int32)
    before = jnp.cumsum(onehot, axis=0) - onehot
    slot_rank = jnp.sum(before * onehot, axis=1)
    slot_index = flat_ids * capacity + slot_rank
    owner_row = jnp.arange(pick_count, dtype=jnp.int32) // per_token
    slot_token = jnp.full((experts * capacity,), tok_rows, jnp.int32).at[slot_index].set(owner_row)
    padded = jnp.concatenate([tokens, jnp.zeros((1, tokens.shape[1]), tokens.dtype)], axis=0)
    returned = expert_block(
        lax.all_gather(
            lax.all_to_all(
                padded[slot_token].reshape(devices_e, local_experts, capacity, tokens.shape[1]),
                "expert",
                split_axis=0,
                concat_axis=0,
                tiled=True,
            ),
            "tensor",
            axis=3,
            tiled=True,
        ),
        w_gate,
        w_up,
        w_down,
    )
    flat_returned = returned.reshape(experts * capacity, returned.shape[3])
    picked = flat_returned[slot_index].reshape(tok_rows, per_token, returned.shape[3])
    weights = gate_fixed.astype(jnp.float32)
    gate_share = weights / jnp.sum(weights, axis=1, keepdims=True)
    mixed_out = jnp.einsum("tk,tkf->tf", gate_share, picked.astype(jnp.float32))
    return mixed_out.astype(jnp.bfloat16)


MESH = pl.DeviceIdType.MESH
VMEM_BYTES = 66_000_000


def fused_kernel(
    tok_rows, feats, experts, hidden_units, E, T,
    x_ref, ids_ref, gates_ref, wg_ref, wu_ref, wd_ref, out_ref,
    ring, down, tok, ids_all, gates_all, acc, hid_t, hid,
    to_partner, from_partner, to_x, from_x, to_z, from_z, own,
    w_sem, d_sem, own_sem, zt_send, zt_recv, zi_send, zi_recv, t_send, t_recv,
    p_send, p_recv, x_send, x_recv, z_send, z_recv,
):
    g, e, t = lax.axis_index("groups"), lax.axis_index("expert"), lax.axis_index("tensor")
    X = T // 2
    x, c = lax.div(t, 2), lax.rem(t, 2)

    def peer(k):
        half, side = (k // 2, k % 2) if isinstance(k, int) else (lax.div(k, 2), lax.rem(k, 2))
        return lax.rem(x + half, X) * 2 + lax.rem(c + side, 2)

    def mirror(k):
        return (-(k // 2)) % X * 2 + k % 2

    def rows_of(block):
        return pl.ds(pl.multiple_of(block * tok_rows, tok_rows), tok_rows)

    def features_of(k):
        return pl.ds(pl.multiple_of(peer(k) * feats, feats), feats)

    pieces = down_pieces(experts, hidden_units)
    piece_rows = experts * hidden_units // pieces

    def weight_copies(k, i):
        slot = (k % 2) * experts + i
        return [
            pltpu.make_async_copy(
                w.at[i, :, features_of(k)],
                ring.at[slot, pl.ds(part * hidden_units, hidden_units), :],
                w_sem.at[slot, part],
            )
            for part, w in enumerate((wg_ref, wu_ref))
        ]

    def down_copy(k, piece):
        rows = pl.ds(pl.multiple_of(piece * piece_rows, piece_rows), piece_rows)
        return pltpu.make_async_copy(
            wd_ref.at[rows, features_of(k)], down.at[k, rows, :], d_sem.at[k, piece]
        )

    for k in range(2):
        @pl.loop(0, experts)
        def _(i, k=k):
            for copy in weight_copies(k, i):
                copy.start()

    barrier = pltpu.get_barrier_semaphore()
    for d in range(1, E):
        pl.semaphore_signal(barrier, inc=1, device_id=(g, lax.rem(e + d, E), t), device_id_type=MESH)
    for k in range(1, T):
        pl.semaphore_signal(barrier, inc=1, device_id=(g, e, peer(k)), device_id_type=MESH)
    pl.semaphore_wait(barrier, E - 1 + T - 1)

    def remote(src, dst, send, recv, where):
        return pltpu.make_async_remote_copy(
            src_ref=src, dst_ref=dst, send_sem=send, recv_sem=recv, device_id=where, device_id_type=MESH
        )

    sent = []

    def go(*args):
        copy = remote(*args)
        copy.start()
        sent.append(copy)

    def arrived(dst, send, recv):
        remote(dst, dst, send, recv, (g, e, peer(1))).wait_recv()

    def spread(source, d):
        block = lax.rem(e + E - d, E)
        for k in [1] + [2 * dx for dx in range(1, X)]:
            m = mirror(k)
            go(source, tok.at[m, rows_of(block), :], t_send.at[k, d], t_recv.at[m, d], (g, e, peer(k)))

    for d in range(1, E):
        where = (g, lax.rem(e + d, E), t)
        go(x_ref, tok.at[0, rows_of(e), :], zt_send.at[d], zt_recv.at[d], where)
    spread(x_ref, 0)
    for d in range(1, E):
        where = (g, lax.rem(e + d, E), t)
        go(ids_ref, ids_all.at[e], zi_send.at[0, d], zi_recv.at[0, d], where)
        go(gates_ref, gates_all.at[e], zi_send.at[1, d], zi_recv.at[1, d], where)
    local = [
        pltpu.make_async_copy(x_ref, tok.at[0, rows_of(e), :], own_sem.at[0]),
        pltpu.make_async_copy(ids_ref, ids_all.at[e], own_sem.at[1]),
        pltpu.make_async_copy(gates_ref, gates_all.at[e], own_sem.at[2]),
    ]
    for copy in local:
        copy.start()
    for d in range(1, E):
        landed = tok.at[0, rows_of(lax.rem(e + E - d, E)), :]
        arrived(landed, zt_send.at[d], zt_recv.at[d])
        spread(landed, d)
    for copy in local:
        copy.wait()

    def project(k, i):
        for copy in weight_copies(k, i):
            copy.wait()
        return lax.dot_general(
            ring[(k % 2) * experts + i], tok[k], (((1,), (1,)), ((), ())), preferred_element_type=jnp.float32
        )

    for k in range(T):
        if k == 1 or (k > 1 and k % 2 == 0):
            for d in range(E):
                block = lax.rem(e + E - d, E)
                landed = tok.at[k, rows_of(block), :]
                arrived(landed, t_send.at[k, d], t_recv.at[k, d])
                if k > 1:
                    go(landed, tok.at[k + 1, rows_of(block), :], t_send.at[k + 1, d], t_recv.at[k + 1, d], (g, e, peer(1)))
        elif k > 1:
            for d in range(E):
                arrived(tok.at[k, rows_of(lax.rem(e + E - d, E)), :], t_send.at[k, d], t_recv.at[k, d])
        if k == T - 1:
            for d in range(1, E):
                s = lax.rem(e + E - d, E)
                arrived(ids_all.at[s], zi_send.at[0, d], zi_recv.at[0, d])
                arrived(gates_all.at[s], zi_send.at[1, d], zi_recv.at[1, d])
            ids = jnp.concatenate([ids_all[s] for s in range(E)], axis=1)
            gates = jnp.concatenate([gates_all[s] for s in range(E)], axis=1).astype(jnp.float32)
            share = gates / jnp.sum(gates, axis=0, keepdims=True)

        @pl.loop(0, experts)
        def _(i, k=k):
            part = project(k, i)
            if k == 0:
                acc[i] = part
            elif k < T - 1:
                acc[i] += part
            else:
                both = acc[i] + part
                gate, up = both[:hidden_units], both[hidden_units:]
                weight = jnp.sum(jnp.where(ids == e * experts + i, share, 0.0), axis=0, keepdims=True)
                value = gate / (1.0 + jnp.exp(-gate)) * up * weight
                hid_t[pl.ds(pl.multiple_of(i * hidden_units, hidden_units), hidden_units), :] = value
            if k + 2 < T:
                for copy in weight_copies(k + 2, i):
                    copy.start()
            if k == 1:
                for n in range(T * pieces // experts):
                    j = i * (T * pieces // experts) + n
                    order = lax.div(j, pieces)
                    down_copy((T - 1) - order, lax.rem(j, pieces)).start()

    pair = 2 * hidden_units

    @pl.loop(0, experts // 2)
    def _(i):
        start = pl.multiple_of(i * pair, pair)
        hid[:, pl.ds(start, pair)] = jnp.transpose(hid_t[pl.ds(start, pair), :]).astype(jnp.bfloat16)

    width = min(256, feats)

    def down_block(k, finish):
        for piece in range(pieces):
            down_copy(k, piece).wait()

        @pl.loop(0, feats // width)
        def _(n):
            columns = pl.ds(pl.multiple_of(n * width, width), width)
            finish(columns, jnp.dot(hid[...], down[k, :, columns], preferred_element_type=jnp.float32))

    after_own = list(range(1, E)) + [0]
    for dx in reversed(range(X)):
        def keep(columns, value, dx=dx):
            to_partner[dx, :, columns] = value.astype(jnp.bfloat16)

        def store(columns, value):
            own[:, columns] = value

        down_block(2 * dx + 1, keep)
        go(to_partner.at[dx], from_partner.at[dx], p_send.at[dx], p_recv.at[dx], (g, e, peer(1)))
        down_block(2 * dx, store)
        arrived(from_partner.at[dx], p_send.at[dx], p_recv.at[dx])
        for j in after_own:
            rows = rows_of(lax.rem(e + j, E))
            total = own[rows, :] + from_partner[dx, rows, :].astype(jnp.float32)
            if dx:
                back = (X - dx) % X
                to_x[dx, rows, :] = total.astype(jnp.bfloat16)
                go(to_x.at[dx, rows, :], from_x.at[back, rows, :], x_send.at[dx, j], x_recv.at[back, j], (g, e, peer(2 * dx)))
                continue
            for other in range(1, X):
                arrived(from_x.at[other, rows, :], x_send.at[other, j], x_recv.at[other, j])
                total += from_x[other, rows, :].astype(jnp.float32)
            if j:
                to_z[j] = total.astype(jnp.bfloat16)
                go(to_z.at[j], from_z.at[j], z_send.at[j], z_recv.at[j], (g, lax.rem(e + j, E), t))
    for d in range(1, E):
        arrived(from_z.at[d], z_send.at[d], z_recv.at[d])
        total += from_z[d].astype(jnp.float32)
    out_ref[...] = total.astype(out_ref.dtype)
    for copy in sent:
        copy.wait_send()


def down_pieces(experts, hidden_units):
    return 4 if experts % 4 == 0 and experts * hidden_units % 64 == 0 else 1


def scratch_of(tok_rows, feats, experts, hidden_units, E, T, per_token):
    bf16, f32, X, N = jnp.bfloat16, jnp.float32, T // 2, E * tok_rows
    dma = pltpu.SemaphoreType.DMA
    return [
        ((2 * experts, 2 * hidden_units, feats), bf16),
        ((T, experts * hidden_units, feats), bf16),
        ((T, N, feats), bf16),
        ((E, per_token, tok_rows), jnp.int32),
        ((E, per_token, tok_rows), jnp.int32),
        ((experts, 2 * hidden_units, N), f32),
        ((experts * hidden_units, N), f32),
        ((N, experts * hidden_units), bf16),
        ((X, N, feats), bf16),
        ((X, N, feats), bf16),
        ((X, N, feats), bf16),
        ((X, N, feats), bf16),
        ((E, tok_rows, feats), bf16),
        ((E, tok_rows, feats), bf16),
        ((N, feats), f32),
    ], [
        dma((2 * experts, 2)), dma((T, down_pieces(experts, hidden_units))), dma((3,)),
        dma((E,)), dma((E,)), dma((2, E)), dma((2, E)), dma((T, E)), dma((T, E)),
        dma((X,)), dma((X,)), dma((X, E)), dma((X, E)), dma((E,)), dma((E,)),
    ]


def fits_fused(sizes):
    tok_rows, feats, experts, hidden_units, E, T, per_token = sizes
    if T % 2 or experts % 4 or E * tok_rows % 128 or feats % 256 or tok_rows % 16:
        return False
    if 2 * hidden_units % 128 or hidden_units % 16 or T * 4 % experts:
        return False
    buffers, _ = scratch_of(*sizes)
    size = 0
    for shape, kind in buffers:
        count = jnp.dtype(kind).itemsize
        for length in shape:
            count *= length
        size += count
    return size < VMEM_BYTES - 2_000_000


def on_device(tokens, expert_ids, gate_fixed, w_gate, w_up, w_down):
    (tok_rows, feats), per_token = tokens.shape, expert_ids.shape[1]
    experts, width, hidden_units = w_gate.shape
    E, T = lax.axis_size("expert"), lax.axis_size("tensor")
    sizes = (tok_rows, feats, experts, hidden_units, E, T, per_token)
    if not fits_fused(sizes):
        return slotted(tokens, expert_ids, gate_fixed, w_gate, w_up, w_down)
    buffers, semaphores = scratch_of(*sizes)
    vmem, anywhere = pl.BlockSpec(memory_space=pltpu.VMEM), pl.BlockSpec(memory_space=pl.ANY)
    return pl.pallas_call(
        functools.partial(fused_kernel, *sizes[:6]),
        out_shape=jax.ShapeDtypeStruct(tokens.shape, tokens.dtype),
        in_specs=[vmem, vmem, vmem, anywhere, anywhere, anywhere],
        out_specs=vmem,
        scratch_shapes=[pltpu.VMEM(shape, kind) for shape, kind in buffers] + semaphores,
        compiler_params=pltpu.CompilerParams(
            collective_id=0, has_side_effects=True, vmem_limit_bytes=VMEM_BYTES
        ),
    )(
        tokens,
        expert_ids.T,
        gate_fixed.T,
        jnp.swapaxes(w_gate, 1, 2),
        jnp.swapaxes(w_up, 1, 2),
        w_down.reshape(experts * hidden_units, width),
    )


def solution(mesh):
    placed = (
        P(("groups", "expert"), "tensor"),
        P(("groups", "expert"), None),
        P(("groups", "expert"), None),
        P("expert", None, "tensor"),
        P("expert", None, "tensor"),
        P("expert", "tensor", None),
    )
    return jax.shard_map(
        on_device,
        mesh=mesh,
        in_specs=placed,
        out_specs=P(("groups", "expert"), "tensor"),
        check_vma=False,
    )
```

```python
import functools

import jax
import jax.numpy as jnp
from jax import lax
from jax.experimental import pallas as pl
from jax.experimental.pallas import tpu as pltpu
from jax.sharding import PartitionSpec as P

CAP = 8


def expert_block(slot_rows, w_gate, w_up, w_down):
    gate_proj = jnp.einsum("gekd,edf->gekf", slot_rows, w_gate, preferred_element_type=jnp.float32)
    up_proj = jnp.einsum("gekd,edf->gekf", slot_rows, w_up, preferred_element_type=jnp.float32)
    hidden = (jax.nn.silu(gate_proj) * up_proj).astype(jnp.bfloat16)
    partial_value = jnp.einsum("gekf,efd->gekd", hidden, w_down, preferred_element_type=jnp.float32)
    summed = lax.psum_scatter(
        partial_value.astype(jnp.bfloat16), "tensor", scatter_dimension=3, tiled=True
    )
    return lax.all_to_all(summed, "expert", split_axis=0, concat_axis=0, tiled=True)


def slotted(tokens, expert_ids, gate_fixed, w_gate, w_up, w_down):
    tok_rows, per_token = expert_ids.shape
    local_experts = w_gate.shape[0]
    devices_e = lax.axis_size("expert")
    experts = local_experts * devices_e
    capacity = CAP
    flat_ids = expert_ids.reshape(-1)
    pick_count = tok_rows * per_token
    onehot = (flat_ids[:, None] == jnp.arange(experts, dtype=jnp.int32)[None, :]).astype(jnp.int32)
    before = jnp.cumsum(onehot, axis=0) - onehot
    slot_rank = jnp.sum(before * onehot, axis=1)
    slot_index = flat_ids * capacity + slot_rank
    owner_row = jnp.arange(pick_count, dtype=jnp.int32) // per_token
    slot_token = jnp.full((experts * capacity,), tok_rows, jnp.int32).at[slot_index].set(owner_row)
    padded = jnp.concatenate([tokens, jnp.zeros((1, tokens.shape[1]), tokens.dtype)], axis=0)
    returned = expert_block(
        lax.all_gather(
            lax.all_to_all(
                padded[slot_token].reshape(devices_e, local_experts, capacity, tokens.shape[1]),
                "expert",
                split_axis=0,
                concat_axis=0,
                tiled=True,
            ),
            "tensor",
            axis=3,
            tiled=True,
        ),
        w_gate,
        w_up,
        w_down,
    )
    flat_returned = returned.reshape(experts * capacity, returned.shape[3])
    picked = flat_returned[slot_index].reshape(tok_rows, per_token, returned.shape[3])
    weights = gate_fixed.astype(jnp.float32)
    gate_share = weights / jnp.sum(weights, axis=1, keepdims=True)
    mixed_out = jnp.einsum("tk,tkf->tf", gate_share, picked.astype(jnp.float32))
    return mixed_out.astype(jnp.bfloat16)


MESH = pl.DeviceIdType.MESH
VMEM_BYTES = 66_000_000
GROUP = 4


def fused_kernel(
    tok_rows, feats, experts, hidden_units, E, T,
    x_ref, ids_ref, gates_ref, wg_ref, wu_ref, wd_ref, out_ref,
    ring, down, tok, ids_all, gates_all, acc, hid_t, hid,
    to_partner, from_partner, to_x, from_x, to_z, from_z, own,
    w_sem, d_sem, own_sem, zt_send, zt_recv, zi_send, zi_recv, t_send, t_recv,
    p_send, p_recv, x_send, x_recv, z_send, z_recv,
):
    g, e, t = lax.axis_index("groups"), lax.axis_index("expert"), lax.axis_index("tensor")
    X = T // 2
    x, c = lax.div(t, 2), lax.rem(t, 2)

    def peer(k):
        half, side = (k // 2, k % 2) if isinstance(k, int) else (lax.div(k, 2), lax.rem(k, 2))
        return lax.rem(x + half, X) * 2 + lax.rem(c + side, 2)

    def mirror(k):
        return (-(k // 2)) % X * 2 + k % 2

    def rows_of(block):
        return pl.ds(pl.multiple_of(block * tok_rows, tok_rows), tok_rows)

    def features_of(k):
        return pl.ds(pl.multiple_of(peer(k) * feats, feats), feats)

    pieces = down_pieces(experts, hidden_units)
    piece_rows = experts * hidden_units // pieces

    def weight_copies(k, i):
        slot = (k % 2) * experts + i
        return [
            pltpu.make_async_copy(
                w.at[i, :, features_of(k)],
                ring.at[slot, pl.ds(part * hidden_units, hidden_units), :],
                w_sem.at[slot, part],
            )
            for part, w in enumerate((wg_ref, wu_ref))
        ]

    def down_copy(k, piece):
        rows = pl.ds(pl.multiple_of(piece * piece_rows, piece_rows), piece_rows)
        return pltpu.make_async_copy(
            wd_ref.at[rows, features_of(k)], down.at[k, rows, :], d_sem.at[k, piece]
        )

    local = [
        pltpu.make_async_copy(x_ref, tok.at[0, rows_of(e), :], own_sem.at[0]),
        pltpu.make_async_copy(ids_ref, ids_all.at[e], own_sem.at[1]),
        pltpu.make_async_copy(gates_ref, gates_all.at[e], own_sem.at[2]),
    ]
    for copy in local:
        copy.start()
    for k in range(2):
        @pl.loop(0, experts)
        def _(i, k=k):
            for copy in weight_copies(k, i):
                copy.start()

    barrier = pltpu.get_barrier_semaphore()
    for d in range(1, E):
        pl.semaphore_signal(barrier, inc=1, device_id=(g, lax.rem(e + d, E), t), device_id_type=MESH)
    for k in range(1, T):
        pl.semaphore_signal(barrier, inc=1, device_id=(g, e, peer(k)), device_id_type=MESH)
    pl.semaphore_wait(barrier, E - 1 + T - 1)

    def remote(src, dst, send, recv, where):
        return pltpu.make_async_remote_copy(
            src_ref=src, dst_ref=dst, send_sem=send, recv_sem=recv, device_id=where, device_id_type=MESH
        )

    for copy in local:
        copy.wait()
    held = tok.at[0, rows_of(e), :]
    sent = []

    def go(*args):
        copy = remote(*args)
        copy.start()
        sent.append(copy)

    def arrived(dst, send, recv):
        remote(dst, dst, send, recv, (g, e, peer(1))).wait_recv()

    def spread(source, d):
        block = lax.rem(e + E - d, E)
        for k in [1] + [2 * dx for dx in range(1, X)]:
            m = mirror(k)
            go(source, tok.at[m, rows_of(block), :], t_send.at[k, d], t_recv.at[m, d], (g, e, peer(k)))

    for d in range(1, E):
        where = (g, lax.rem(e + d, E), t)
        go(held, held, zt_send.at[d], zt_recv.at[d], where)
    spread(held, 0)
    for d in range(1, E):
        where = (g, lax.rem(e + d, E), t)
        go(ids_all.at[e], ids_all.at[e], zi_send.at[0, d], zi_recv.at[0, d], where)
        go(gates_all.at[e], gates_all.at[e], zi_send.at[1, d], zi_recv.at[1, d], where)
    for d in range(1, E):
        landed = tok.at[0, rows_of(lax.rem(e + E - d, E)), :]
        arrived(landed, zt_send.at[d], zt_recv.at[d])
        spread(landed, d)
    def project(k, i):
        for n in range(GROUP):
            for copy in weight_copies(k, i + n):
                copy.wait()
        rows = ring[pl.ds((k % 2) * experts + i, GROUP)].reshape(GROUP * 2 * hidden_units, feats)
        return lax.dot_general(rows, tok[k], (((1,), (1,)), ((), ())), preferred_element_type=jnp.float32)

    for k in range(T):
        if k == 1 or (k > 1 and k % 2 == 0):
            for d in range(E):
                block = lax.rem(e + E - d, E)
                landed = tok.at[k, rows_of(block), :]
                arrived(landed, t_send.at[k, d], t_recv.at[k, d])
                if k > 1:
                    go(landed, tok.at[k + 1, rows_of(block), :], t_send.at[k + 1, d], t_recv.at[k + 1, d], (g, e, peer(1)))
        elif k > 1:
            for d in range(E):
                arrived(tok.at[k, rows_of(lax.rem(e + E - d, E)), :], t_send.at[k, d], t_recv.at[k, d])
        if k == T - 1:
            for d in range(1, E):
                s = lax.rem(e + E - d, E)
                arrived(ids_all.at[s], zi_send.at[0, d], zi_recv.at[0, d])
                arrived(gates_all.at[s], zi_send.at[1, d], zi_recv.at[1, d])
            ids = jnp.concatenate([ids_all[s] for s in range(E)], axis=1)
            gates = jnp.concatenate([gates_all[s] for s in range(E)], axis=1).astype(jnp.float32)
            share = gates / jnp.sum(gates, axis=0, keepdims=True)

        @pl.loop(0, experts // GROUP)
        def _(step, k=k):
            i = step * GROUP
            parts = project(k, i).reshape(GROUP, 2 * hidden_units, -1)
            for n in range(GROUP):
                if k == 0:
                    acc[i + n] = parts[n]
                elif k < T - 1:
                    acc[i + n] += parts[n]
                else:
                    both = acc[i + n] + parts[n]
                    gate, up = both[:hidden_units], both[hidden_units:]
                    weight = jnp.sum(jnp.where(ids == e * experts + i + n, share, 0.0), axis=0, keepdims=True)
                    value = gate / (1.0 + jnp.exp(-gate)) * up * weight
                    start = pl.multiple_of((i + n) * hidden_units, hidden_units)
                    hid_t[pl.ds(start, hidden_units), :] = value
            if k + 2 < T:
                for n in range(GROUP):
                    for copy in weight_copies(k + 2, i + n):
                        copy.start()
            if k == 1:
                for n in range(GROUP * T * pieces // experts):
                    j = step * (GROUP * T * pieces // experts) + n
                    order = lax.div(j, pieces)
                    down_copy((T - 1) - order, lax.rem(j, pieces)).start()

    pair = 2 * hidden_units

    @pl.loop(0, experts // 2)
    def _(i):
        start = pl.multiple_of(i * pair, pair)
        hid[:, pl.ds(start, pair)] = jnp.transpose(hid_t[pl.ds(start, pair), :]).astype(jnp.bfloat16)

    width = 256

    parts_n = feats // width

    def down_part(k, n):
        if n == 0:
            for piece in range(pieces):
                down_copy(k, piece).wait()
        return jnp.dot(
            hid[...], down[k, :, n * width:(n + 1) * width], preferred_element_type=jnp.float32
        )

    def meet_partner(dx, n):
        value = down_part(2 * dx, n)
        arrived(from_partner.at[dx, n], p_send.at[dx, n], p_recv.at[dx, n])
        return value + from_partner[dx, n].astype(jnp.float32)

    for dx in reversed(range(X)):
        for n in range(parts_n + 1):
            if n < parts_n:
                to_partner[dx, n] = down_part(2 * dx + 1, n).astype(jnp.bfloat16)
                go(to_partner.at[dx, n], from_partner.at[dx, n], p_send.at[dx, n], p_recv.at[dx, n], (g, e, peer(1)))
            if n and dx:
                back, m = (X - dx) % X, n - 1
                to_x[dx, m] = meet_partner(dx, m).astype(jnp.bfloat16)
                go(to_x.at[dx, m], from_x.at[back, m], x_send.at[dx, m], x_recv.at[back, m], (g, e, peer(2 * dx)))
            elif n:
                own[n - 1] = meet_partner(0, n - 1)
    for n in range(parts_n):
        for other in range(1, X):
            arrived(from_x.at[other, n], x_send.at[other, n], x_recv.at[other, n])
            own[n] += from_x[other, n].astype(jnp.float32)
        for j in range(1, E):
            to_z[j, n] = own[n, rows_of(lax.rem(e + j, E)), :].astype(jnp.bfloat16)
            go(to_z.at[j, n], from_z.at[j, n], z_send.at[j, n], z_recv.at[j, n], (g, lax.rem(e + j, E), t))
    for n in range(parts_n):
        total = own[n, rows_of(e), :]
        for d in range(1, E):
            arrived(from_z.at[d, n], z_send.at[d, n], z_recv.at[d, n])
            total += from_z[d, n].astype(jnp.float32)
        out_ref[:, n * width:(n + 1) * width] = total.astype(out_ref.dtype)
    for copy in sent:
        copy.wait_send()


def down_pieces(experts, hidden_units):
    return 4 if experts % 4 == 0 and experts * hidden_units % 64 == 0 else 1


def scratch_of(tok_rows, feats, experts, hidden_units, E, T, per_token):
    bf16, f32, X, N = jnp.bfloat16, jnp.float32, T // 2, E * tok_rows
    width, parts_n = 256, feats // 256
    dma = pltpu.SemaphoreType.DMA
    return [
        ((2 * experts, 2 * hidden_units, feats), bf16),
        ((T, experts * hidden_units, feats), bf16),
        ((T, N, feats), bf16),
        ((E, per_token, tok_rows), jnp.int32),
        ((E, per_token, tok_rows), jnp.int32),
        ((experts, 2 * hidden_units, N), f32),
        ((experts * hidden_units, N), f32),
        ((N, experts * hidden_units), bf16),
        ((X, parts_n, N, width), bf16),
        ((X, parts_n, N, width), bf16),
        ((X, parts_n, N, width), bf16),
        ((X, parts_n, N, width), bf16),
        ((E, parts_n, tok_rows, width), bf16),
        ((E, parts_n, tok_rows, width), bf16),
        ((parts_n, N, width), f32),
    ], [
        dma((2 * experts, 2)), dma((T, down_pieces(experts, hidden_units))), dma((3,)),
        dma((E,)), dma((E,)), dma((2, E)), dma((2, E)), dma((T, E)), dma((T, E)),
        dma((X, parts_n)), dma((X, parts_n)), dma((X, parts_n)), dma((X, parts_n)), dma((E, parts_n)), dma((E, parts_n)),
    ]


def fits_fused(sizes):
    tok_rows, feats, experts, hidden_units, E, T, per_token = sizes
    if T % 2 or experts % GROUP or experts % 4 or E * tok_rows % 128 or feats % 256 or tok_rows % 16:
        return False
    if 2 * hidden_units % 128 or hidden_units % 16 or T * 4 % experts:
        return False
    buffers, _ = scratch_of(*sizes)
    size = 0
    for shape, kind in buffers:
        count = jnp.dtype(kind).itemsize
        for length in shape:
            count *= length
        size += count
    return size < VMEM_BYTES - 2_000_000


def on_device(tokens, expert_ids, gate_fixed, w_gate, w_up, w_down):
    (tok_rows, feats), per_token = tokens.shape, expert_ids.shape[1]
    experts, width, hidden_units = w_gate.shape
    E, T = lax.axis_size("expert"), lax.axis_size("tensor")
    sizes = (tok_rows, feats, experts, hidden_units, E, T, per_token)
    if not fits_fused(sizes):
        return slotted(tokens, expert_ids, gate_fixed, w_gate, w_up, w_down)
    buffers, semaphores = scratch_of(*sizes)
    vmem, anywhere = pl.BlockSpec(memory_space=pltpu.VMEM), pl.BlockSpec(memory_space=pl.ANY)
    return pl.pallas_call(
        functools.partial(fused_kernel, *sizes[:6]),
        out_shape=jax.ShapeDtypeStruct(tokens.shape, tokens.dtype),
        in_specs=[anywhere] * 6,
        out_specs=vmem,
        scratch_shapes=[pltpu.VMEM(shape, kind) for shape, kind in buffers] + semaphores,
        compiler_params=pltpu.CompilerParams(
            collective_id=0, has_side_effects=True, vmem_limit_bytes=VMEM_BYTES
        ),
    )(
        tokens,
        expert_ids.T,
        gate_fixed.T,
        jnp.swapaxes(w_gate, 1, 2),
        jnp.swapaxes(w_up, 1, 2),
        w_down.reshape(experts * hidden_units, width),
    )


def solution(mesh):
    placed = (
        P(("groups", "expert"), "tensor"),
        P(("groups", "expert"), None),
        P(("groups", "expert"), None),
        P("expert", None, "tensor"),
        P("expert", None, "tensor"),
        P("expert", "tensor", None),
    )
    return jax.shard_map(
        on_device,
        mesh=mesh,
        in_specs=placed,
        out_specs=P(("groups", "expert"), "tensor"),
        check_vma=False,
    )
```
